32 devices in a mesh: pop: 8 (over z, y), tp: 4 (over x, core).
Axes of the slice: x: 2, y: 2, z: 4, core: 2. Of those that a mesh axis runs over, the one named last changes fastest.
Arguments:
- tokens: bfloat16 [8192, 5120], P('pop', 'tp'), may hold values from -6 to 6
- target: bfloat16 [8192, 5120], P('pop', 'tp'), may hold values from -6 to 6
- weight: bfloat16 [5120, 5120], P('pop', 'tp'), may hold values from -6 to 6
- factor_out: bfloat16 [32, 4, 5120], P('pop'), may hold values from -6 to 6
- factor_in: bfloat16 [32, 4, 5120], P('pop', None, 'tp'), may hold values from -6 to 6
Outputs:
- perturbed: bfloat16 [8192, 5120], P('pop', 'tp')
- new_weight: bfloat16 [5120, 5120], P('pop', 'tp')
The draws below stay inside these ranges and needn't reach their ends.
All inputs are finite; a program needn't handle non-finite values.
Results may differ from the reference program's by a relative error of at most 0.012.
Values may be sent and summed in bfloat16 or wider, within the bound.
No kernel may reach another device: no remote copies, remote signals or barrier semaphores. Data moves between devices by JAX's collectives and lax.ppermute only.
A program may use at most 128 MiB of HBM per device.

```python
import math
import jax
import jax.numpy as jnp
from jax import lax

D_IN = 5120
D_OUT = 5120
R = 4
TOK_MEM = 256
MEMBERS = 32
TOKENS = 8192
N_TP = 4


def level_of(own_key, extent, shards, least, top_value):
    factor_of, own = 1.0, jax.random.fold_in(own_key, 6)
    for dim, parts in shards:
        draws = jnp.exp(jax.random.uniform(jax.random.fold_in(own, dim), (parts,), jnp.float32, least / len(shards), top_value / len(shards)))
        factor_of = factor_of * jnp.repeat(draws, extent[dim] // parts).reshape([-1 if axis == dim else 1 for axis in range(len(extent))])
    return factor_of


def gaussian(stream_key, extent, width, reach, split=(), held_as=jnp.bfloat16):
    array = jax.random.normal(stream_key, extent, jnp.float32) * width
    if len(split) > 0:
        array = level_of(stream_key, extent, split, -0.22, 0.18) * array
    return jnp.clip(array, min=-reach, max=reach).astype(held_as)


def setup_inputs(seed: int = 0) -> dict:
    splits = jax.random.split(jax.random.key(seed), 6)
    tokens = gaussian(splits[0], (TOKENS, D_IN), 1.0, 6.0, ((0, 8), (1, 4)))
    target = gaussian(splits[1], (TOKENS, D_OUT), 1.0, 6.0, ((0, 8), (1, 4)))
    weight = gaussian(splits[2], (D_OUT, D_IN), 1.0, 6.0, ((0, 8), (1, 4)))
    factor_out = gaussian(splits[3], (MEMBERS, R, D_OUT), 1.0, 6.0, ((0, 8),))
    factor_in = gaussian(splits[4], (MEMBERS, R, D_IN), 1.0, 6.0, ((0, 8), (2, 4)))
    return dict(tokens=tokens, target=target, weight=weight, factor_out=factor_out, factor_in=factor_in)


noise_scale = 0.25
step_scale = 10.0

def reference(tokens, target, weight, factor_out, factor_in):
    shard_width = D_IN // N_TP
    token_sets = tokens.reshape(MEMBERS, TOK_MEM, D_IN)
    target_sets = target.reshape(MEMBERS, TOK_MEM, D_OUT)

    def member(member_parts):
        inputs, wanted, outer, inner = member_parts
        total = jnp.zeros((TOK_MEM, D_OUT), jnp.float32)
        for block in range(N_TP):
            lower = block * shard_width
            upper = lower + shard_width
            partial_value = jnp.dot(inputs[:, lower:upper], weight[:, lower:upper].T, preferred_element_type=jnp.float32) / math.sqrt(D_IN)
            total = total + lax.optimization_barrier(partial_value.astype(jnp.bfloat16)).astype(jnp.float32)
        codes_all = jnp.dot(inputs.astype(jnp.float32), inner.astype(jnp.float32).T, precision=lax.Precision.HIGHEST)
        low_rank = jnp.dot(codes_all, outer.astype(jnp.float32), precision=lax.Precision.HIGHEST) * (noise_scale / math.sqrt(R * D_IN))
        output_full = total + low_rank
        fitness_one = jnp.sum(output_full * wanted.astype(jnp.float32)) / (TOK_MEM * math.sqrt(D_OUT))
        return (output_full.astype(jnp.bfloat16), fitness_one)
    outputs, fitness = lax.map(member, (token_sets, target_sets, factor_out, factor_in))
    centered = fitness - jnp.mean(fitness)
    scaled = (centered[:, None, None] * factor_out.astype(jnp.float32)).astype(jnp.bfloat16)
    delta = jnp.dot(scaled.reshape(MEMBERS * R, D_OUT).T, factor_in.reshape(MEMBERS * R, D_IN), preferred_element_type=jnp.float32)
    updated = (weight.astype(jnp.float32) + step_scale / math.sqrt(MEMBERS * R) * delta).astype(jnp.bfloat16)
    return (outputs.reshape(TOKENS, D_OUT), updated)
```

```python
import math

import jax
import jax.numpy as jnp
from jax import lax
from jax.experimental import pallas as pl
from jax.experimental.pallas import tpu as pltpu
from jax.sharding import PartitionSpec as P


noise_scale = 0.25
step_scale = 10.0

AXES = ("pop", "tp")
LINE = 4
LANES = 128


def plain(tokens, target, weight, factor_out, factor_in):
    tok_rows, shard_width = tokens.shape
    mem_local, rank, width_out = factor_out.shape
    tok_member = tok_rows // mem_local
    tp_count = lax.axis_size("tp")
    width_in = shard_width * tp_count
    out_cols = width_out // tp_count
    col_first = lax.axis_index("tp") * out_cols
    base_factor = 1.0 / math.sqrt(width_in)
    token_sets = tokens.reshape(mem_local, tok_member, shard_width)
    codes_part = jnp.einsum(
        "mkc,mrc->mkr", token_sets, factor_in, preferred_element_type=jnp.float32
    )
    codes_sum = lax.psum(codes_part, "tp")
    partial_terms = (
        lax.dot_general(
            tokens,
            lax.all_gather(weight, "pop", axis=0, tiled=True),
            (((1,), (1,)), ((), ())),
            preferred_element_type=jnp.float32,
        )
        * base_factor
    )
    base_sum = lax.psum_scatter(
        partial_terms.astype(jnp.bfloat16), "tp", scatter_dimension=1, tiled=True
    ).astype(jnp.float32)
    outer_cols = lax.dynamic_slice_in_dim(factor_out, col_first, out_cols, 2).astype(jnp.float32)
    low_rank = jnp.einsum(
        "mkr,mrc->mkc", codes_sum, outer_cols, precision=lax.Precision.HIGHEST
    ) * (noise_scale / math.sqrt(rank * width_in))
    output_full = base_sum.reshape(mem_local, tok_member, out_cols) + low_rank
    wanted = target.reshape(mem_local, tok_member, out_cols).astype(jnp.float32)
    fitness_part = jnp.sum(output_full * wanted, axis=(1, 2)) / (tok_member * math.sqrt(width_out))
    fitness_local = lax.psum(fitness_part, "tp")
    fitness_all = lax.all_gather(fitness_local, "pop", axis=0, tiled=True)
    outer_rows = lax.all_to_all(factor_out, "pop", split_axis=2, concat_axis=0, tiled=True)
    inner_cols = lax.all_gather(factor_in, "pop", axis=0, tiled=True)
    centered = fitness_all - jnp.mean(fitness_all)
    scaled = (centered[:, None, None] * outer_rows.astype(jnp.float32)).astype(jnp.bfloat16)
    delta = jnp.einsum("imo,imc->oc", scaled, inner_cols, preferred_element_type=jnp.float32)
    members_all = fitness_all.shape[0]
    updated = (
        weight.astype(jnp.float32) + step_scale / math.sqrt(members_all * rank) * delta
    ).astype(jnp.bfloat16)
    return (output_full.reshape(tok_rows, out_cols).astype(jnp.bfloat16), updated)


def send(array, rule):
    pairs = []
    for z in range(LINE):
        for y in range(2):
            for x in range(2):
                for c in range(2):
                    to = rule(z, y, x, c)
                    if to is not None:
                        tz, ty, tx, tc = to
                        pairs.append(
                            (((z * 2 + y) * 2 + x) * 2 + c, ((tz * 2 + ty) * 2 + tx) * 2 + tc)
                        )
    return lax.ppermute(array, AXES, pairs)


def keep_core(z, x, step):
    return ((z % 2) if x == z // 2 else (z // 2)) ^ step


def cuts(rows):
    blocks = rows // LANES
    wide = max(1, (blocks - 1) // 2)
    edges = sorted({0, wide * LANES, (blocks - 1) * LANES, blocks * LANES})
    return tuple(zip(edges[:-1], edges[1:]))


def contract(left, right):
    return lax.dot_general(left, right, (((1,), (1,)), ((), ())), preferred_element_type=jnp.float32)


def finish_body(count, flags, *refs):
    totals, sides, others = (refs[2 * count * g : 2 * count * (g + 1)] for g in range(3))
    low_ref, want_ref, out_ref, fit_ref = refs[6 * count :]
    half = pl.program_id(1)

    def emit(group):
        base = jnp.concatenate([ref[...] for ref in group], axis=1)
        value = base.astype(jnp.float32) + low_ref[...]
        out_ref[...] = value.astype(out_ref.dtype)
        product = value * want_ref[...].astype(jnp.float32)
        rows, cols = product.shape
        folded = product.reshape(rows // 8, 8, cols).sum(axis=0)
        lanes = sum(folded[:, lo : lo + LANES] for lo in range(0, cols, LANES))

        @pl.when(half == 0)
        def _():
            fit_ref[0] = lanes

        @pl.when(half == 1)
        def _():
            fit_ref[0] += lanes

    for step in range(2):
        here = flags[0] == step
        part = slice(step * count, (step + 1) * count)

        @pl.when(here & (half == 0) & (flags[1] == 0))
        def _():
            emit(totals[part])

        @pl.when(here & (half == 0) & (flags[1] == 1))
        def _():
            emit(sides[part])

        @pl.when(here & (half == 1))
        def _():
            emit(others[part])


def finish(flags, totals, sides, others, low_rank, target, members):
    rows, width = low_rank.shape
    block = rows // members
    count = len(totals) // 2

    def column(m, h, flags):
        own = flags[2]
        return (m, jnp.where(h == 0, own, 1 - own))

    def spec(array, want):
        return pl.BlockSpec(
            (block, array.shape[1]), lambda m, h, flags: (jnp.where(want(flags), m, 0), 0)
        )

    specs = []
    for group, side in ((totals, 0), (sides, 1), (others, None)):
        for i, array in enumerate(group):
            step = i // count
            if side is None:
                specs.append(spec(array, lambda f, s=step: f[0] == s))
            else:
                specs.append(spec(array, lambda f, s=step, d=side: (f[0] == s) & (f[1] == d)))
    specs += [pl.BlockSpec((block, width // 2), column)] * 2
    return pl.pallas_call(
        lambda flags, *refs: finish_body(count, flags, *refs),
        grid_spec=pltpu.PrefetchScalarGridSpec(
            num_scalar_prefetch=1,
            grid=(members, 2),
            in_specs=specs,
            out_specs=[
                pl.BlockSpec((block, width // 2), column),
                pl.BlockSpec((1, 8, LANES), lambda m, h, flags: (m, 0, 0)),
            ],
        ),
        out_shape=[
            jax.ShapeDtypeStruct((rows, width), target.dtype),
            jax.ShapeDtypeStruct((members, 8, LANES), jnp.float32),
        ],
        cost_estimate=pl.CostEstimate(
            flops=4 * rows * width, bytes_accessed=12 * rows * width, transcendentals=0
        ),
        compiler_params=pltpu.CompilerParams(vmem_limit_bytes=16 * 1024 * 1024),
    )(flags, *totals, *sides, *others, low_rank, target)


def local(tokens, target, weight, factor_out, factor_in):
    return split_step(tokens, target, weight, factor_out, factor_in)


def split_step(tokens, target, weight, factor_out, factor_in):
    tok_rows, shard_width = tokens.shape
    mem_local, rank, width_out = factor_out.shape
    weight_rows = weight.shape[0]
    tok_member = tok_rows // mem_local
    tp_count = lax.axis_size("tp")
    pop_count = lax.axis_size("pop")
    width_in = shard_width * tp_count
    out_cols = width_out // tp_count
    base_factor = 1.0 / math.sqrt(width_in)
    pop, tp = lax.axis_index("pop"), lax.axis_index("tp")
    z, y, x, c = pop // 2, pop % 2, tp // 2, tp % 2
    inner = (z == 1) | (z == 2)
    near_first = x == z // 2
    bit = jnp.where(near_first, z % 2, z // 2)
    flags = jnp.stack([c ^ bit, c, y]).astype(jnp.int32)
    pieces = cuts(weight_rows)
    count = len(pieces)
    sub = lambda array: [array[lo:hi] for lo, hi in pieces]

    partner = lambda z, y, x, c: (z, y, x, 1 - c)

    mid = lambda z, y, x, c: (3 - z, y, x, c) if z in (1, 2) else None
    end = lambda z, y, x, c: (z ^ 1, y, x, c) if z in (1, 2) else None
    swap = send(weight, lambda z, y, x, c: (z ^ 1, y, x, c))
    early = [lax.optimization_barrier(sub(weight)), lax.optimization_barrier(sub(swap))]
    early_o = [send(weight, partner), send(swap, partner)]
    rows_a = send(tokens, lambda z, y, x, c: (z, 1 - y, x, 1) if c == 0 else None)
    rows_p = send(tokens, partner)
    rows_b = send(tokens, lambda z, y, x, c: (z, 1 - y, x, 1) if c == 1 else None)
    at_mid = [[send(early[s][k], mid) for k in range(count)] for s in range(2)]
    at_end = [[send(at_mid[s][k], end) for k in range(count)] for s in range(2)]
    rows_a, rows_b = jnp.where(c == 0, rows_p, rows_a), jnp.where(c == 0, tokens, rows_b)

    outer_flat = factor_out.reshape(mem_local * rank, width_out)
    inner_flat = factor_in.reshape(mem_local * rank, shard_width)
    payload = jnp.concatenate(
        [
            outer_flat.reshape(mem_local * rank, pop_count, weight_rows).transpose(1, 0, 2),
            jnp.broadcast_to(inner_flat[None], (pop_count,) + inner_flat.shape),
        ],
        axis=2,
    )
    factors = lax.all_to_all(payload, "pop", split_axis=0, concat_axis=0, tiled=True)
    factors = factors.reshape(pop_count * mem_local * rank, weight_rows + shard_width)

    token_sets = tokens.reshape(mem_local, tok_member, shard_width)
    codes = jnp.einsum("mkc,mrc->mrk", token_sets, factor_in, preferred_element_type=jnp.float32)
    codes = codes.reshape(mem_local * rank, tok_member)
    codes = codes + send(codes, lambda z, y, x, c: (z, y, x, 1 - c))
    codes = codes + send(codes, lambda z, y, x, c: (z, y, 1 - x, c))
    codes = codes.reshape(mem_local, rank, tok_member)
    outer_cols = lax.dynamic_slice_in_dim(factor_out, tp * out_cols, out_cols, 2).astype(jnp.float32)
    low_rank = jnp.einsum(
        "mrk,mrc->mkc", codes, outer_cols, precision=lax.Precision.HIGHEST
    ) * (noise_scale / math.sqrt(rank * width_in))
    low_rank = low_rank.reshape(tok_rows, out_cols)

    rows_a, rows_b, low_rank, factors = lax.optimization_barrier((rows_a, rows_b, low_rank, factors))
    outer_rows, inner_cols = factors[:, :weight_rows], factors[:, weight_rows:]
    early_sum = [[None] * count, [None] * count]
    for step in range(2):
        for k, (lo, hi) in enumerate(pieces):
            early_sum[step][k] = contract(rows_b, early[step][k]) + contract(
                rows_a, early_o[step][lo:hi]
            )
    totals, sides, others = [], [], []
    for step in range(2):
        for k in range(count):
            last = jnp.where(inner, at_mid[step][k], at_end[step][k])
            last_o = send(last, partner)
            last_sum = contract(rows_b, last) + contract(rows_a, last_o)
            far_sum = jnp.where(near_first, last_sum, early_sum[step][k]) * base_factor
            near_sum = jnp.where(near_first, early_sum[step][k], last_sum) * base_factor
            far_sum = far_sum.astype(jnp.bfloat16)
            moved = send(far_sum, lambda z, y, x, c: (z, y, 1 - x, c))
            total = (near_sum + moved.astype(jnp.float32)).astype(jnp.bfloat16)
            totals.append(total)
            sides.append(send(total, partner))
            others.append(
                send(
                    total,
                    lambda z, y, x, c: (z, 1 - y, x, keep_core(z, x, step)) if c == 1 else None,
                )
            )

    out, fits = finish(flags, totals, sides, others, low_rank, target, mem_local)
    fitness_part = jnp.sum(fits, axis=(1, 2)) / (tok_member * math.sqrt(width_out))
    members_all = pop_count * mem_local
    slots = jnp.arange(members_all) // mem_local == pop
    fitness_all = jnp.where(slots, jnp.tile(fitness_part, pop_count), 0.0)
    for rule in (
        lambda z, y, x, c: (z, y, x, 1 - c),
        lambda z, y, x, c: (z, y, 1 - x, c),
        lambda z, y, x, c: (z, 1 - y, x, c),
        lambda z, y, x, c: (z ^ 1, y, x, c),
        lambda z, y, x, c: (3 - z, y, x, c),
    ):
        fitness_all = fitness_all + send(fitness_all, rule)
    centered = fitness_all - jnp.mean(fitness_all)
    scaled = (jnp.repeat(centered, rank)[:, None] * outer_rows.astype(jnp.float32)).astype(jnp.bfloat16)
    delta = lax.dot_general(
        scaled, inner_cols, (((0,), (0,)), ((), ())), preferred_element_type=jnp.float32
    )
    updated = (
        weight.astype(jnp.float32) + step_scale / math.sqrt(members_all * rank) * delta
    ).astype(jnp.bfloat16)
    return (out, updated)


def solution(mesh):
    in_specs = (
        P("pop", "tp"),
        P("pop", "tp"),
        P("pop", "tp"),
        P("pop", None, None),
        P("pop", None, "tp"),
    )
    out_specs = (P("pop", "tp"), P("pop", "tp"))
    split = mesh.shape["pop"] == 2 * LINE and mesh.shape["tp"] == 4
    body = local if split else plain
    return jax.shard_map(body, mesh=mesh, in_specs=in_specs, out_specs=out_specs, check_vma=False)
```

```python
import math

import jax
import jax.numpy as jnp
from jax import lax
from jax.experimental import pallas as pl
from jax.experimental.pallas import tpu as pltpu
from jax.sharding import PartitionSpec as P


noise_scale = 0.25
step_scale = 10.0

AXES = ("pop", "tp")
LINE = 4
LANES = 128
VMEM_GRANT = 24 * 1024 * 1024


def plain(tokens, target, weight, factor_out, factor_in):
    tok_rows, shard_width = tokens.shape
    mem_local, rank, width_out = factor_out.shape
    tok_member = tok_rows // mem_local
    tp_count = lax.axis_size("tp")
    width_in = shard_width * tp_count
    out_cols = width_out // tp_count
    col_first = lax.axis_index("tp") * out_cols
    base_factor = 1.0 / math.sqrt(width_in)
    token_sets = tokens.reshape(mem_local, tok_member, shard_width)
    codes_part = jnp.einsum(
        "mkc,mrc->mkr", token_sets, factor_in, preferred_element_type=jnp.float32
    )
    codes_sum = lax.psum(codes_part, "tp")
    partial_terms = (
        lax.dot_general(
            tokens,
            lax.all_gather(weight, "pop", axis=0, tiled=True),
            (((1,), (1,)), ((), ())),
            preferred_element_type=jnp.float32,
        )
        * base_factor
    )
    base_sum = lax.psum_scatter(
        partial_terms.astype(jnp.bfloat16), "tp", scatter_dimension=1, tiled=True
    ).astype(jnp.float32)
    outer_cols = lax.dynamic_slice_in_dim(factor_out, col_first, out_cols, 2).astype(jnp.float32)
    low_rank = jnp.einsum(
        "mkr,mrc->mkc", codes_sum, outer_cols, precision=lax.Precision.HIGHEST
    ) * (noise_scale / math.sqrt(rank * width_in))
    output_full = base_sum.reshape(mem_local, tok_member, out_cols) + low_rank
    wanted = target.reshape(mem_local, tok_member, out_cols).astype(jnp.float32)
    fitness_part = jnp.sum(output_full * wanted, axis=(1, 2)) / (tok_member * math.sqrt(width_out))
    fitness_local = lax.psum(fitness_part, "tp")
    fitness_all = lax.all_gather(fitness_local, "pop", axis=0, tiled=True)
    outer_rows = lax.all_to_all(factor_out, "pop", split_axis=2, concat_axis=0, tiled=True)
    inner_cols = lax.all_gather(factor_in, "pop", axis=0, tiled=True)
    centered = fitness_all - jnp.mean(fitness_all)
    scaled = (centered[:, None, None] * outer_rows.astype(jnp.float32)).astype(jnp.bfloat16)
    delta = jnp.einsum("imo,imc->oc", scaled, inner_cols, preferred_element_type=jnp.float32)
    members_all = fitness_all.shape[0]
    updated = (
        weight.astype(jnp.float32) + step_scale / math.sqrt(members_all * rank) * delta
    ).astype(jnp.bfloat16)
    return (output_full.reshape(tok_rows, out_cols).astype(jnp.bfloat16), updated)


def send(array, rule):
    pairs = []
    for z in range(LINE):
        for y in range(2):
            for x in range(2):
                for c in range(2):
                    to = rule(z, y, x, c)
                    if to is not None:
                        tz, ty, tx, tc = to
                        pairs.append(
                            (((z * 2 + y) * 2 + x) * 2 + c, ((tz * 2 + ty) * 2 + tx) * 2 + tc)
                        )
    return lax.ppermute(array, AXES, pairs)


def keep_core(z, x, step):
    return ((z % 2) if x == z // 2 else (z // 2)) ^ step


def cuts(rows):
    narrow = rows // LANES // 2 * LANES
    return ((0, narrow), (narrow, rows)), ((0, narrow), (narrow, rows - LANES), (rows - LANES, rows))


def contract(left, right):
    return lax.dot_general(left, right, (((1,), (1,)), ((), ())), preferred_element_type=jnp.float32)


def choose(flags, half, totals, sides, others, emit):
    for step in range(2):
        here = flags[0] == step

        @pl.when(here & (half == 0) & (flags[1] == 0))
        def _():
            emit(step, totals[step])

        @pl.when(here & (half == 0) & (flags[1] == 1))
        def _():
            emit(step, sides[step])

        @pl.when(here & (half == 1))
        def _():
            emit(step, others[step])


def fold(product):
    rows, cols = product.shape
    folded = product.reshape(rows // 8, 8, cols).sum(axis=0)
    return sum(folded[:, lo : lo + LANES] for lo in range(0, cols, LANES))


def needed(step, side):
    if side is None:
        return lambda flags: flags[0] == step
    return lambda flags: (flags[0] == step) & (flags[1] == side)


def finish_most(flags, totals, sides, others, low_rank, target, members):
    rows, width = target.shape
    together = 2 if members % 2 == 0 else 1
    block, half_width = rows // members * together, width // 2
    groups = [group for step in range(2) for group in ((0, totals[step]), (1, sides[step]), (None, others[step]))]

    def body(flags, *refs):
        picked, at = [], 0
        for _, arrays in groups:
            picked.append(refs[at : at + len(arrays)])
            at += len(arrays)
        low_ref, want_ref, out_ref, fit_ref = refs[at:]
        half = pl.program_id(1)

        def emit(step, group):
            parts = [ref[...] for ref in group]
            have = sum(part.shape[1] for part in parts)
            if have < half_width:
                parts.append(jnp.zeros((block, half_width - have), parts[0].dtype))
            value = jnp.concatenate(parts, axis=1).astype(jnp.float32)
            value += low_ref[...].astype(jnp.float32)
            out_ref[...] = value.astype(out_ref.dtype)
            product = value * want_ref[...].astype(jnp.float32)
            size = block // together
            for m in range(together):
                lanes = fold(product[m * size : (m + 1) * size])

                @pl.when(half == 0)
                def _():
                    fit_ref[m] = lanes

                @pl.when(half == 1)
                def _():
                    fit_ref[m] += lanes

        choose(flags, half, picked[0::3], picked[1::3], picked[2::3], emit)

    def column(m, h, flags):
        return (m, jnp.where(h == 0, flags[2], 1 - flags[2]))

    specs, operands = [], []
    for i, (side, arrays) in enumerate(groups):
        want = needed(i // 3, side)
        for array in arrays:
            specs.append(
                pl.BlockSpec(
                    (block, array.shape[1]),
                    lambda m, h, flags, want=want: (jnp.where(want(flags), m, 0), 0),
                )
            )
            operands.append(array)
    specs += [pl.BlockSpec((block, half_width), column)] * 2
    return pl.pallas_call(
        body,
        grid_spec=pltpu.PrefetchScalarGridSpec(
            num_scalar_prefetch=1,
            grid=(members // together, 2),
            in_specs=specs,
            out_specs=[
                pl.BlockSpec((block, half_width), column),
                pl.BlockSpec((together, 8, LANES), lambda m, h, flags: (m, 0, 0)),
            ],
        ),
        out_shape=[
            jax.ShapeDtypeStruct((rows, width), target.dtype),
            jax.ShapeDtypeStruct((members, 8, LANES), jnp.float32),
        ],
        cost_estimate=pl.CostEstimate(
            flops=4 * rows * width, bytes_accessed=12 * rows * width, transcendentals=0
        ),
        compiler_params=pltpu.CompilerParams(vmem_limit_bytes=VMEM_GRANT),
    )(flags, *operands, low_rank, target)


def finish_last(flags, piece, totals, sides, others, low_rank, target, members, out):
    lo, hi = piece
    rows, width = target.shape
    half_blocks, first = width // 2 // LANES, lo // LANES
    operands = [array for step in range(2) for array in (totals[step], sides[step], others[step])]

    def body(flags, *refs):
        low_ref, want_ref, _, out_ref, fit_ref = refs[6:]

        @pl.when((pl.program_id(0) == 0) & (pl.program_id(1) == 0))
        def _():
            fit_ref[...] = jnp.zeros_like(fit_ref)

        def emit(step, ref):
            base = ref[...].astype(jnp.float32)
            out_ref[...] = (base + low_ref[...].astype(jnp.float32)).astype(out_ref.dtype)
            if step == 1:
                product = base * want_ref[...].astype(jnp.float32)
                size = rows // members
                for m in range(members):
                    fit_ref[m] += fold(product[m * size : (m + 1) * size])

        choose(flags, pl.program_id(1), refs[0:6:3], refs[1:6:3], refs[2:6:3], emit)

    def column(j, h, flags):
        return (0, jnp.where(h == 0, flags[2], 1 - flags[2]) * half_blocks + first + j)

    specs = []
    for i, array in enumerate(operands):
        want = needed(i // 3, (0, 1, None)[i % 3])
        start = (array.shape[1] - (hi - lo)) // LANES
        specs.append(
            pl.BlockSpec(
                (rows, LANES),
                lambda j, h, flags, want=want, start=start: (0, jnp.where(want(flags), start + j, 0)),
            )
        )
    specs += [
        pl.BlockSpec((rows, LANES), column),
        pl.BlockSpec((rows, LANES), column),
        pl.BlockSpec(memory_space=pl.ANY),
    ]
    return pl.pallas_call(
        body,
        grid_spec=pltpu.PrefetchScalarGridSpec(
            num_scalar_prefetch=1,
            grid=((hi - lo) // LANES, 2),
            in_specs=specs,
            out_specs=[
                pl.BlockSpec((rows, LANES), column),
                pl.BlockSpec((members, 8, LANES), lambda j, h, flags: (0, 0, 0)),
            ],
        ),
        out_shape=[
            jax.ShapeDtypeStruct((rows, width), out.dtype),
            jax.ShapeDtypeStruct((members, 8, LANES), jnp.float32),
        ],
        input_output_aliases={9: 0},
        cost_estimate=pl.CostEstimate(
            flops=4 * rows * (hi - lo), bytes_accessed=20 * rows * (hi - lo), transcendentals=0
        ),
        compiler_params=pltpu.CompilerParams(vmem_limit_bytes=VMEM_GRANT),
    )(flags, *operands, low_rank, target, out)


def local(tokens, target, weight, factor_out, factor_in):
    return split_step(tokens, target, weight, factor_out, factor_in)


def split_step(tokens, target, weight, factor_out, factor_in):
    tok_rows, shard_width = tokens.shape
    mem_local, rank, width_out = factor_out.shape
    weight_rows = weight.shape[0]
    tok_member = tok_rows // mem_local
    tp_count = lax.axis_size("tp")
    pop_count = lax.axis_size("pop")
    width_in = shard_width * tp_count
    out_cols = width_out // tp_count
    base_factor = 1.0 / math.sqrt(width_in)
    pop, tp = lax.axis_index("pop"), lax.axis_index("tp")
    z, y, x, c = pop // 2, pop % 2, tp // 2, tp % 2
    inner = (z == 1) | (z == 2)
    near_first = x == z // 2
    bit = jnp.where(near_first, z % 2, z // 2)
    flags = jnp.stack([c ^ bit, c, y]).astype(jnp.int32)
    pieces = cuts(weight_rows)
    sub = lambda array, step: [array[lo:hi] for lo, hi in pieces[step]]

    partner = lambda z, y, x, c: (z, y, x, 1 - c)

    mid = lambda z, y, x, c: (3 - z, y, x, c) if z in (1, 2) else None
    end = lambda z, y, x, c: (z ^ 1, y, x, c) if z in (1, 2) else None
    swap = send(weight, lambda z, y, x, c: (z ^ 1, y, x, c))
    early = [lax.optimization_barrier(sub(weight, 0)), lax.optimization_barrier(sub(swap, 1))]
    early_o = [send(weight, partner), send(swap, partner)]
    rows_a = send(tokens, lambda z, y, x, c: (z, 1 - y, x, 1) if c == 0 else None)
    rows_p = send(tokens, partner)
    rows_b = send(tokens, lambda z, y, x, c: (z, 1 - y, x, 1) if c == 1 else None)
    at_mid = [[send(w, mid) for w in early[s]] for s in range(2)]
    at_end = [[send(w, end) for w in at_mid[s]] for s in range(2)]
    rows = jnp.concatenate(
        [jnp.where(c == 0, tokens, rows_b), jnp.where(c == 0, rows_p, rows_a)], axis=1
    )

    outer_flat = factor_out.reshape(mem_local * rank, width_out)
    inner_flat = factor_in.reshape(mem_local * rank, shard_width)
    payload = jnp.concatenate(
        [
            outer_flat.reshape(mem_local * rank, pop_count, weight_rows).transpose(1, 0, 2),
            jnp.broadcast_to(inner_flat[None], (pop_count,) + inner_flat.shape),
        ],
        axis=2,
    )
    token_sets = tokens.reshape(mem_local, tok_member, shard_width)
    codes = jnp.einsum("mkc,mrc->mrk", token_sets, factor_in, preferred_element_type=jnp.float32)
    codes = codes.reshape(mem_local * rank, tok_member)
    codes = codes + send(codes, lambda z, y, x, c: (z, y, x, 1 - c))
    codes = codes + send(codes, lambda z, y, x, c: (z, y, 1 - x, c))
    codes = codes.reshape(mem_local, rank, tok_member)
    outer_cols = lax.dynamic_slice_in_dim(factor_out, tp * out_cols, out_cols, 2).astype(jnp.float32)
    low_rank = jnp.einsum(
        "mrk,mrc->mkc", codes, outer_cols, precision=lax.Precision.HIGHEST
    ) * (noise_scale / math.sqrt(rank * width_in))
    low_rank = low_rank.astype(target.dtype).reshape(tok_rows, out_cols)

    rows, low_rank, payload = lax.optimization_barrier((rows, low_rank, payload))
    factors = lax.all_to_all(payload, "pop", split_axis=0, concat_axis=0, tiled=True)
    factors = factors.reshape(pop_count * mem_local * rank, weight_rows + shard_width)
    early_sum = [[None] * len(part) for part in pieces]
    for step in range(2):
        for k, (lo, hi) in enumerate(pieces[step]):
            block = jnp.concatenate([early[step][k], early_o[step][lo:hi]], axis=1)
            early_sum[step][k] = contract(rows, block)
    totals, sides, others = ([], []), ([], []), ([], [])
    for step in range(2):
        for k in range(len(pieces[step])):
            last = jnp.where(inner, at_mid[step][k], at_end[step][k])
            last_o = send(last, partner)
            last_sum = contract(rows, jnp.concatenate([last, last_o], axis=1))
            far_sum = jnp.where(near_first, last_sum, early_sum[step][k]) * base_factor
            near_sum = jnp.where(near_first, early_sum[step][k], last_sum) * base_factor
            far_sum = far_sum.astype(jnp.bfloat16)
            moved = send(far_sum, lambda z, y, x, c: (z, y, 1 - x, c))
            total = (near_sum + moved.astype(jnp.float32)).astype(jnp.bfloat16)
            totals[step].append(total)
            sides[step].append(send(total, partner))
            others[step].append(
                send(
                    total,
                    lambda z, y, x, c: (z, 1 - y, x, keep_core(z, x, step)) if c == 1 else None,
                )
            )

    outer_rows, inner_cols = factors[:, :weight_rows], factors[:, weight_rows:]
    most = lambda arrays: (arrays[0], arrays[1][:-1])
    out, fits = finish_most(
        flags, most(totals), most(sides), most(others), low_rank, target, mem_local
    )
    tail = lambda arrays: (arrays[0][-1], arrays[1][-1])
    out, last_fits = finish_last(
        flags,
        pieces[1][-1],
        tail(totals),
        tail(sides),
        tail(others),
        low_rank,
        target,
        mem_local,
        out,
    )
    fitness_part = jnp.sum(fits + last_fits, axis=(1, 2)) / (tok_member * math.sqrt(width_out))
    members_all = pop_count * mem_local
    slots = jnp.arange(members_all) // mem_local == pop
    fitness_all = jnp.where(slots, jnp.tile(fitness_part, pop_count), 0.0)
    for rule in (
        lambda z, y, x, c: (z, y, x, 1 - c),
        lambda z, y, x, c: (z, y, 1 - x, c),
        lambda z, y, x, c: (z, 1 - y, x, c),
        lambda z, y, x, c: (z ^ 1, y, x, c),
        lambda z, y, x, c: (3 - z, y, x, c),
    ):
        fitness_all = fitness_all + send(fitness_all, rule)
    centered = fitness_all - jnp.mean(fitness_all)
    scaled = (jnp.repeat(centered, rank)[:, None] * outer_rows.astype(jnp.float32)).astype(jnp.bfloat16)
    delta = lax.dot_general(
        scaled, inner_cols, (((0,), (0,)), ((), ())), preferred_element_type=jnp.float32
    )
    updated = (
        weight.astype(jnp.float32) + step_scale / math.sqrt(members_all * rank) * delta
    ).astype(jnp.bfloat16)
    return (out, updated)


def solution(mesh):
    in_specs = (
        P("pop", "tp"),
        P("pop", "tp"),
        P("pop", "tp"),
        P("pop", None, None),
        P("pop", None, "tp"),
    )
    out_specs = (P("pop", "tp"), P("pop", "tp"))
    split = mesh.shape["pop"] == 2 * LINE and mesh.shape["tp"] == 4
    body = local if split else plain
    return jax.shard_map(body, mesh=mesh, in_specs=in_specs, out_specs=out_specs, check_vma=False)
```
